32 devices in a mesh: mem: 8 (over z, x), geo: 4 (over y, core).
Axes of the slice: x: 2, y: 2, z: 4, core: 2. Of those that a mesh axis runs over, the one named last changes fastest.
Arguments:
- control: float32 [8, 32, 48, 384], P('mem', 'geo'), may hold values from -6 to 6
- kappa_table: float32 [16], replicated, may hold values from 0.02 to 0.24
- kappa_index: int32 [48, 384], replicated, may hold values from 0 to 15
- tile_bounds: int32 [5], replicated, may hold values from 0 to 18432, as said below
- filter_bands: float32 [4, 5, 32], replicated, may hold values from -0.3 to 0.3
- perturbation: bfloat16 [2, 8, 32, 18432], P(None, 'mem', None, 'geo'), may hold values from -6 to 6
Outputs:
- increment: float32 [2, 32, 18432], P(None, 'mem', 'geo')
The draws below stay inside these ranges and needn't reach their ends.
Inputs may be any that keep to these rules, and one draw needn't show every extreme that they name: tile_bounds[0] is 0, tile_bounds[4] is 18432, and the bounds never fall; tile t holds columns tile_bounds[t] to tile_bounds[t + 1] - 1.
All inputs are finite; a program needn't handle non-finite values.
Results may differ from the reference program's by a relative error of at most 0.005.
Values may be sent and summed in bfloat16 or wider, within the bound.
A program may use at most 64 MiB of HBM per device.

```python
import math
import jax
import jax.numpy as jnp
from jax import lax

LEV = 32
HX = 48
HY = 384
ITERS = 10
KAPPAS = 16
MEMBERS = 8
TILES = 4
NCOL = 18432


def draw_tile_bounds(key, part):
    widths = jax.random.randint(jax.random.fold_in(key, 7), (TILES,), 1, 5)
    cumulative = jnp.cumsum(widths).astype(jnp.int32)
    interior = HX * HY * cumulative // cumulative[-1]
    return jnp.concatenate([jnp.zeros((1,), jnp.int32), interior.astype(jnp.int32)])


def plant(array, key, least, largest):
    longest = array.shape.index(max(array.shape))
    spots = []
    for shift in (0, 1):
        where = [jax.random.randint(jax.random.fold_in(key, axis), (), 0, length) for axis, length in enumerate(array.shape)]
        where[longest] = (where[longest] + shift) % array.shape[longest]
        spots.append(tuple(where))
    return array.at[spots[0]].set(least).at[spots[1]].set(largest)


def raised(array, rng, source, target, parts, factor):
    owner, partner = [(jnp.arange(array.shape[position]) // (array.shape[position] // parts)).reshape([-1 if axis == position else 1 for axis in range(array.ndim)]) for position in (source, target)]
    chosen = jax.random.permutation(rng, parts)[partner]
    strong = (owner == chosen) | (owner == (partner + parts // 2) % parts)
    return jnp.where(strong, factor * array, array)


def shard_levels(own_key, dims, shards, least, high):
    gain = 1.0
    for axis_at, blocks in shards:
        steps = jax.random.uniform(jax.random.fold_in(jax.random.fold_in(own_key, 6), axis_at), (blocks,), jnp.float32, least / len(shards), high / len(shards))
        gain = gain * jnp.repeat(jnp.exp(steps), dims[axis_at] // blocks).reshape((-1,) + (1,) * (len(dims) - 1 - axis_at))
    return gain


def normal_values(stream_key, dims, spread, reach, cuts=(), kind=jnp.bfloat16):
    level = shard_levels(stream_key, dims, cuts, -0.22, 0.18) if cuts else 1.0
    entries = jax.random.normal(stream_key, dims, jnp.float32) * spread * level
    return jnp.minimum(jnp.maximum(entries, -reach), reach).astype(kind)


def heavy_noise(stream_key, extent, width, limit, pieces, heavy, kind=jnp.bfloat16):
    values = width * jax.random.normal(stream_key, extent, jnp.float32)
    if pieces:
        values = values * shard_levels(stream_key, extent, pieces, -0.22, 0.18)
    return jnp.clip(raised(values, jax.random.fold_in(stream_key, 3), *heavy), -limit, limit).astype(kind)


def setup_inputs(seed: int = 0) -> dict:
    keys = jax.random.split(jax.random.key(seed), 7)
    control = normal_values(keys[0], (MEMBERS, LEV, HX, HY), 1.0, 6.0, ((0, 8), (1, 4)), jnp.float32)
    kappa_table = jnp.clip(jnp.exp(jax.random.uniform(keys[1], (KAPPAS,), jnp.float32, math.log(0.02), math.log(0.24))), 0.02, 0.24)
    kappa_index = plant(jax.random.randint(keys[2], (HX, HY), 0, KAPPAS), jax.random.fold_in(keys[2], 1), 0, KAPPAS - 1).astype(jnp.int32)
    tile_bounds = draw_tile_bounds(jax.random.fold_in(keys[6], 71), 0)
    filter_bands = jnp.clip(jax.random.uniform(keys[4], (TILES, 5, LEV), jnp.float32, -0.3, 0.3), -0.3, 0.3)
    perturbation = heavy_noise(keys[5], (2, MEMBERS, LEV, NCOL), 1.0, 6.0, ((1, 8), (3, 4)), (1, 2, 8, 2.0))
    return {"control": control, "kappa_table": kappa_table, "kappa_index": kappa_index, "tile_bounds": tile_bounds, "filter_bands": filter_bands, "perturbation": perturbation}


def neighbours(state):
    east = jnp.concatenate([state[..., 1:, :], state[..., -1:, :]], axis=-2)
    west = jnp.concatenate([state[..., :1, :], state[..., :-1, :]], axis=-2)
    north = jnp.concatenate([state[..., 1:], state[..., -1:]], axis=-1)
    south = jnp.concatenate([state[..., :1], state[..., :-1]], axis=-1)
    return east, west, north, south


def face_weights(kappa_field):
    return tuple(0.5 * (kappa_field + other) for other in neighbours(kappa_field))


def diffuse_step(state, weights):
    east, west, north, south = neighbours(state)
    update = weights[0] * (east - state) + weights[1] * (west - state)
    update = update + weights[2] * (north - state) + weights[3] * (south - state)
    return state + update


def vertical_filter(values, coefficients):
    levels = values.shape[0]
    padded = jnp.pad(values, ((2, 2), (0, 0)))
    result = values
    for offset in range(5):
        result = result + coefficients[offset] * padded[offset:offset + levels]
    return result


def reference(control, kappa_table, kappa_index, tile_bounds, filter_bands, perturbation):
    kappa_field = kappa_table[kappa_index]
    weights = face_weights(kappa_field)
    columns = jnp.arange(HX * HY, dtype=jnp.int32)
    tile_ids = jnp.sum((columns[None, :] >= tile_bounds[1:-1][:, None]).astype(jnp.int32), axis=0).astype(jnp.int32)
    coefficients = jnp.transpose(filter_bands[tile_ids], (1, 2, 0))

    def one_member(member_field):
        state_field = lax.fori_loop(0, ITERS, lambda step, cur: diffuse_step(cur, weights), member_field)
        flattened = state_field.reshape(LEV, HX * HY)
        return vertical_filter(flattened, coefficients).astype(jnp.bfloat16)

    filtered = lax.map(one_member, control)

    def accumulate(running, members_pair):
        member_filtered, member_pert = members_pair
        return running + member_pert.astype(jnp.float32) * member_filtered.astype(jnp.float32)[None], None

    running, unused = lax.scan(accumulate, jnp.zeros((2, LEV, HX * HY), jnp.float32), (filtered, jnp.moveaxis(perturbation, 1, 0)))
    return running
```

```python
import functools

import jax
import jax.numpy as jnp
from jax import lax
from jax.experimental import pallas as pl
from jax.experimental.pallas import tpu as pltpu
from jax.sharding import PartitionSpec as P

ITERS = 10
F32, BF16 = jnp.float32, jnp.bfloat16
LANES = 128


def kernel(nm, ng, ctrl, table, kidx_hbm, bounds, bands_hbm, pert_hbm, out,
           S, WE, WN, kidx, kf, bands, bandsb, coef, pert, PS, PR, B, G, D, FS, FR,
           loc_sem, ps_sem, pr_sem, gs_sem, gr_sem, fs_sem, fr_sem):
    mem = lax.axis_index("mem")
    geo = lax.axis_index("geo")
    hx, lev, hy = S.shape
    nvar, levels, cols = pert.shape
    lm = levels // nm
    rows = hx // ng
    tiles, nband, _ = bands.shape
    pad = nband // 2

    barrier = pltpu.get_barrier_semaphore()
    for d in range(1, nm):
        pl.semaphore_signal(barrier, inc=1, device_id={"mem": lax.rem(mem + d, nm)}, device_id_type=pl.DeviceIdType.MESH)
    for d in range(1, ng):
        pl.semaphore_signal(barrier, inc=1, device_id={"geo": lax.rem(geo + d, ng)}, device_id_type=pl.DeviceIdType.MESH)

    pert_cp = pltpu.make_async_copy(pert_hbm.at[:, 0], pert, loc_sem.at[0])
    pert_cp.start()
    kidx_cp = pltpu.make_async_copy(kidx_hbm, kidx, loc_sem.at[1])
    kidx_cp.start()
    bands_cp = pltpu.make_async_copy(bands_hbm, bands, loc_sem.at[2])
    bands_cp.start()
    ctrl_cps = []
    for l in range(lev):
        cp = pltpu.make_async_copy(ctrl.at[0, l], S.at[:, l], loc_sem.at[3 + l])
        cp.start()
        ctrl_cps.append(cp)

    pert_cp.wait()

    def repack(q, carry):
        at = pl.ds(pl.multiple_of(q * LANES, LANES), LANES)
        vals = [pert[v, :, at].astype(F32) for v in range(nvar)]
        for m in range(nm):
            piece = jnp.concatenate([v[m * lm:(m + 1) * lm] for v in vals], axis=0)
            PS[m, :, at] = piece.astype(BF16)
        return carry

    lax.fori_loop(0, cols // LANES, repack, 0)
    pl.semaphore_wait(barrier, nm - 1 + ng - 1)

    def exchange(src, dst, send, recv, axis, me, d, n):
        peer = lax.rem(me + d, n)
        return pltpu.make_async_remote_copy(
            src_ref=src(peer), dst_ref=dst, send_sem=send.at[d], recv_sem=recv.at[d],
            device_id={axis: peer}, device_id_type=pl.DeviceIdType.MESH)

    pert_ex = [exchange(lambda p: PS.at[p], PR.at[d], ps_sem, pr_sem, "mem", mem, d, nm) for d in range(1, nm)]
    for cp in pert_ex:
        cp.start()

    kidx_cp.wait()
    index = kidx[...]
    field = jnp.zeros(index.shape, F32)
    for entry in range(table.shape[0]):
        field = jnp.where(index == entry, table[entry], field)
    kf[...] = field
    inner = lax.broadcasted_iota(jnp.int32, (1, hy), 1) < hy - 1

    def weights(i, carry):
        own = kf[pl.ds(i, 1), :]
        after = kf[pl.ds(jnp.minimum(i + 1, hx - 1), 1), :]
        WE[i] = jnp.broadcast_to(0.5 * (own + after), (lev, hy))
        north = jnp.where(inner, 0.5 * (own + pltpu.roll(own, hy - 1, axis=1)), 0.0)
        WN[i] = jnp.broadcast_to(north, (lev, hy))
        return carry

    lax.fori_loop(0, hx, weights, 0)

    def sweep(write):
        s, before = S[0], None
        for i in range(hx):
            fn = WN[i] * (pltpu.roll(s, hy - 1, axis=1) - s)
            new = s + (fn - pltpu.roll(fn, 1, axis=1))
            if before is not None:
                new = new - before
            if i < hx - 1:
                after = S[i + 1]
                before = WE[i] * (after - s)
                new = new + before
                s = after
            write(i, new)

    def keep(i, new):
        S[i] = new

    def narrow(i, new):
        B[i] = new.astype(BF16)

    for cp in ctrl_cps:
        cp.wait()

    def step(it, carry):
        sweep(keep)
        return carry

    lax.fori_loop(0, ITERS - 1, step, 0)
    sweep(narrow)

    geo_ex = [exchange(lambda p: B.at[pl.ds(p * rows, rows)], G.at[geo], gs_sem, gr_sem, "geo", geo, d, ng)
              for d in range(1, ng)]
    for cp in geo_ex:
        cp.start()
    own_geo = pltpu.make_async_copy(B.at[pl.ds(geo * rows, rows)], G.at[geo], gr_sem.at[0])
    own_geo.start()

    bands_cp.wait()
    eye = (lax.broadcasted_iota(jnp.int32, (levels, levels), 0)
           == lax.broadcasted_iota(jnp.int32, (levels, levels), 1))
    for t in range(tiles):
        for k in range(nband):
            row = jnp.broadcast_to(bands[t, k:k + 1, :], (levels, levels))
            column = jnp.sum(jnp.where(eye, row, 0.0), axis=1, keepdims=True)
            bandsb[t, k] = jnp.broadcast_to(column, (levels, LANES))

    def coefficients(q, carry):
        at = pl.ds(pl.multiple_of(q * LANES, LANES), LANES)
        column = geo * cols + q * LANES + lax.broadcasted_iota(jnp.int32, (levels, LANES), 1)
        past = [column >= bounds[t] for t in range(1, tiles)]
        for k in range(nband):
            value = bandsb[0, k]
            for t in range(1, tiles):
                value = jnp.where(past[t - 1], bandsb[t, k], value)
            coef[k, :, at] = value
        return carry

    lax.fori_loop(0, cols // LANES, coefficients, 0)
    base = 8
    D[0:base, :] = jnp.zeros((base, cols), F32)
    D[base + levels:, :] = jnp.zeros((D.shape[0] - base - levels, cols), F32)

    own_geo.wait()
    for cp in geo_ex:
        cp.wait_recv()
    for g in range(ng):
        for r in range(rows):
            D[base + g * lev:base + (g + 1) * lev, r * hy:(r + 1) * hy] = G[g, r].astype(F32)

    def vertical(q, carry):
        at = pl.ds(pl.multiple_of(q * LANES, LANES), LANES)
        value = D[base:base + levels, at]
        for k in range(nband):
            value = value + coef[k, :, at] * D[base + k - pad:base + k - pad + levels, at]
        for m in range(nm):
            FS[m, :, at] = value[m * lm:(m + 1) * lm].astype(BF16)
        return carry

    lax.fori_loop(0, cols // LANES, vertical, 0)
    filt_ex = [exchange(lambda p: FS.at[p], FR.at[d], fs_sem, fr_sem, "mem", mem, d, nm) for d in range(1, nm)]
    for cp in filt_ex:
        cp.start()
    own_filt = pltpu.make_async_copy(FS.at[mem], FR.at[0], fr_sem.at[0])
    own_filt.start()
    own_pert = pltpu.make_async_copy(PS.at[mem], PR.at[0], pr_sem.at[0])
    own_pert.start()
    own_pert.wait()
    own_filt.wait()
    for cp in pert_ex:
        cp.wait_recv()
    for cp in filt_ex:
        cp.wait_recv()

    def total(q, carry):
        at = pl.ds(pl.multiple_of(q * LANES, LANES), LANES)
        acc = jnp.zeros((nvar * lm, LANES), F32)
        for m in range(nm):
            f = FR[m, :, at].astype(F32)
            acc = acc + PR[m, :, at].astype(F32) * jnp.concatenate([f] * nvar, axis=0)
        for v in range(nvar):
            out[v, :, at] = acc[v * lm:(v + 1) * lm]
        return carry

    lax.fori_loop(0, cols // LANES, total, 0)
    for cp in pert_ex + geo_ex + filt_ex:
        cp.wait_send()


def body(nm, ng, control, kappa_table, kappa_index, tile_bounds, filter_bands, perturbation):
    _, lev, hx, hy = control.shape
    nvar, _, levels, cols = perturbation.shape
    lm = levels // nm
    rows = hx // ng
    tiles, nband, _ = filter_bands.shape
    dma = pltpu.SemaphoreType.DMA
    hbm = pl.BlockSpec(memory_space=pl.ANY)
    smem = pl.BlockSpec(memory_space=pltpu.SMEM)
    return pl.pallas_call(
        functools.partial(kernel, nm, ng),
        out_shape=jax.ShapeDtypeStruct((nvar, lm, cols), F32),
        in_specs=[hbm, smem, hbm, smem, hbm, hbm],
        out_specs=pl.BlockSpec(memory_space=pltpu.VMEM),
        scratch_shapes=[
            pltpu.VMEM((hx, lev, hy), F32),
            pltpu.VMEM((hx, lev, hy), F32),
            pltpu.VMEM((hx, lev, hy), F32),
            pltpu.VMEM((hx, hy), jnp.int32),
            pltpu.VMEM((hx, hy), F32),
            pltpu.VMEM((tiles, nband, levels), F32),
            pltpu.VMEM((tiles, nband, levels, LANES), F32),
            pltpu.VMEM((nband, levels, cols), F32),
            pltpu.VMEM((nvar, levels, cols), BF16),
            pltpu.VMEM((nm, nvar * lm, cols), BF16),
            pltpu.VMEM((nm, nvar * lm, cols), BF16),
            pltpu.VMEM((hx, lev, hy), BF16),
            pltpu.VMEM((ng, rows, lev, hy), BF16),
            pltpu.VMEM((levels + 16, cols), F32),
            pltpu.VMEM((nm, lm, cols), BF16),
            pltpu.VMEM((nm, lm, cols), BF16),
            dma((3 + lev,)), dma((nm,)), dma((nm,)), dma((ng,)), dma((ng,)), dma((nm,)), dma((nm,)),
        ],
        compiler_params=pltpu.CompilerParams(
            collective_id=0, has_side_effects=True, vmem_limit_bytes=56 * 2**20),
    )(control, kappa_table, kappa_index, tile_bounds, filter_bands, perturbation)


def solution(mesh):
    in_specs = (P("mem", "geo", None, None), P(), P(), P(), P(), P(None, "mem", None, "geo"))
    out_specs = P(None, "mem", "geo")
    run = functools.partial(body, mesh.shape["mem"], mesh.shape["geo"])
    return jax.shard_map(run, mesh=mesh, in_specs=in_specs, out_specs=out_specs, check_vma=False)
```

```python
import functools

import jax
import jax.numpy as jnp
from jax import lax
from jax.experimental import pallas as pl
from jax.experimental.pallas import tpu as pltpu
from jax.sharding import PartitionSpec as P

ITERS = 10
F32, BF16 = jnp.float32, jnp.bfloat16
LANES = 128


def kernel(nm, ng, ctrl, table_hbm, kidx_hbm, bounds_hbm, bands_hbm, pert_hbm, out,
           table, bounds, S, WE, WN, WS, spread, gather, kidx, kf, bands, bandsb, coef, pert, PS, PR, B, G, D, FS, FR,
           loc_sem, ps_sem, pr_sem, gs_sem, gr_sem, fs_sem, fr_sem):
    mem = lax.axis_index("mem")
    geo = lax.axis_index("geo")
    hx, lev, hy = S.shape
    nvar, levels, cols = pert.shape
    lm = levels // nm
    rows = hx // ng
    nband, tiles, _ = bands.shape
    parts = hy // LANES
    pad = nband // 2

    barrier = pltpu.get_barrier_semaphore()
    for d in range(1, nm):
        pl.semaphore_signal(barrier, inc=1, device_id={"mem": lax.rem(mem + d, nm)}, device_id_type=pl.DeviceIdType.MESH)
    for d in range(1, ng):
        pl.semaphore_signal(barrier, inc=1, device_id={"geo": lax.rem(geo + d, ng)}, device_id_type=pl.DeviceIdType.MESH)

    pert_cp = pltpu.make_async_copy(pert_hbm.at[:, 0], pert, loc_sem.at[0])
    pert_cp.start()
    kidx_cp = pltpu.make_async_copy(kidx_hbm, kidx, loc_sem.at[1])
    kidx_cp.start()
    bands_cp = pltpu.make_async_copy(bands_hbm, bands, loc_sem.at[2])
    bands_cp.start()
    table_cp = pltpu.make_async_copy(table_hbm, table, loc_sem.at[3])
    table_cp.start()
    bounds_cp = pltpu.make_async_copy(bounds_hbm, bounds, loc_sem.at[4])
    bounds_cp.start()
    ctrl_cps = []
    for l in range(lev):
        cp = pltpu.make_async_copy(ctrl.at[0, l], S.at[:, l], loc_sem.at[5 + l])
        cp.start()
        ctrl_cps.append(cp)

    left = lax.broadcasted_iota(jnp.int32, (hy, hy), 0)
    right = lax.broadcasted_iota(jnp.int32, (hy, hy), 1)
    spread[...] = jnp.where(left == (right % LANES) * parts + right // LANES, 1.0, 0.0).astype(BF16)
    gather[...] = jnp.where(right == (left % LANES) * parts + left // LANES, 1.0, 0.0).astype(BF16)

    pert_cp.wait()

    def repack(q, carry):
        at = pl.ds(pl.multiple_of(q * hy, LANES), hy)
        vals = [pert[v, :, at].astype(F32) for v in range(nvar)]
        for m in range(nm):
            piece = jnp.concatenate([v[m * lm:(m + 1) * lm] for v in vals], axis=0)
            PS[m, :, at] = piece.astype(BF16)
        return carry

    lax.fori_loop(0, cols // hy, repack, 0)
    pl.semaphore_wait(barrier, nm - 1 + ng - 1)

    def exchange(src, dst, send, recv, axis, me, d, n):
        peer = lax.rem(me + d, n)
        return pltpu.make_async_remote_copy(
            src_ref=src(peer), dst_ref=dst, send_sem=send.at[d], recv_sem=recv.at[d],
            device_id={axis: peer}, device_id_type=pl.DeviceIdType.MESH)

    pert_ex = [exchange(lambda p: PS.at[p], PR.at[d], ps_sem, pr_sem, "mem", mem, d, nm) for d in range(1, nm)]
    for cp in pert_ex:
        cp.start()

    kidx_cp.wait()
    table_cp.wait()
    index = jnp.dot(kidx[...].astype(F32).astype(BF16), spread[...], preferred_element_type=F32)
    field = jnp.zeros(index.shape, F32)
    for entry in range(table.shape[0]):
        field = jnp.where(index == float(entry), table[entry], field)
    kf[0:hx] = field
    kf[hx:] = jnp.zeros((kf.shape[0] - hx, hy), F32)
    east = 0.5 * (field + kf[1:hx + 1])
    lane = lax.broadcasted_iota(jnp.int32, (hx, LANES), 1)
    cut = [field[:, p * LANES:(p + 1) * LANES] for p in range(parts)]
    norths = [0.5 * (cut[p] + cut[p + 1]) for p in range(parts - 1)]
    last = 0.5 * (cut[-1] + pltpu.roll(cut[0], LANES - 1, axis=1))
    norths.append(jnp.where(lane < LANES - 1, last, 0.0))
    south = pltpu.roll(norths[-1], 1, axis=1)
    for i in range(hx):
        if i < hx - 1:
            WE[i] = jnp.broadcast_to(east[i:i + 1], (lev, hy))
        for p in range(parts):
            WN[i, :, p * LANES:(p + 1) * LANES] = jnp.broadcast_to(norths[p][i:i + 1], (lev, LANES))
        WS[i] = jnp.broadcast_to(south[i:i + 1], (lev, LANES))

    for cp in ctrl_cps:
        cp.wait()
    group = rows if (rows * lev) % 8 == 0 else hx
    for i in range(0, hx, group):
        x = S[i:i + group].reshape(group * lev, hy)
        high = x.astype(BF16)
        low = (x - high.astype(F32)).astype(BF16)
        x = (jnp.dot(high, spread[...], preferred_element_type=F32)
             + jnp.dot(low, spread[...], preferred_element_type=F32))
        S[i:i + group] = x.reshape(group, lev, hy)

    def step(it, carry):
        s = [S[0, :, p * LANES:(p + 1) * LANES] for p in range(parts)]
        before = None
        for i in range(hx):
            wn = [WN[i, :, p * LANES:(p + 1) * LANES] for p in range(parts)]
            ahead = s[1:] + [pltpu.roll(s[0], LANES - 1, axis=1)]
            flux = [wn[p] * (ahead[p] - s[p]) for p in range(parts)]
            behind = [WS[i] * (s[0] - pltpu.roll(s[-1], 1, axis=1))] + flux[:-1]
            new = [s[p] + (flux[p] - behind[p]) for p in range(parts)]
            if before is not None:
                new = [new[p] - before[p] for p in range(parts)]
            if i < hx - 1:
                after = [S[i + 1, :, p * LANES:(p + 1) * LANES] for p in range(parts)]
                before = [WE[i, :, p * LANES:(p + 1) * LANES] * (after[p] - s[p]) for p in range(parts)]
                new = [new[p] + before[p] for p in range(parts)]
                s = after
            for p in range(parts):
                S[i, :, p * LANES:(p + 1) * LANES] = new[p]
        return carry

    lax.fori_loop(0, ITERS, step, 0)
    for i in range(0, hx, group):
        x = S[i:i + group].reshape(group * lev, hy).astype(BF16)
        x = jnp.dot(x, gather[...], preferred_element_type=F32)
        B[i:i + group] = x.reshape(group, lev, hy).astype(BF16)

    geo_ex = [exchange(lambda p: B.at[pl.ds(p * rows, rows)], G.at[geo], gs_sem, gr_sem, "geo", geo, d, ng)
              for d in range(1, ng)]
    for cp in geo_ex:
        cp.start()
    own_geo = pltpu.make_async_copy(B.at[pl.ds(geo * rows, rows)], G.at[geo], gr_sem.at[0])
    own_geo.start()

    bands_cp.wait()
    bounds_cp.wait()
    eye = (lax.broadcasted_iota(jnp.int32, (levels, levels), 0)
           == lax.broadcasted_iota(jnp.int32, (levels, levels), 1))
    for t in range(tiles):
        for k in range(nband):
            row = jnp.broadcast_to(bands[k, t:t + 1, :], (levels, levels))
            column = jnp.sum(jnp.where(eye, row, 0.0), axis=1, keepdims=True)
            bandsb[t, k] = jnp.broadcast_to(column, (levels, LANES))

    def coefficients(q, carry):
        at = pl.ds(pl.multiple_of(q * LANES, LANES), LANES)
        column = geo * cols + q * LANES + lax.broadcasted_iota(jnp.int32, (levels, LANES), 1)
        past = [column >= bounds[t] for t in range(1, tiles)]
        for k in range(nband):
            value = bandsb[0, k]
            for t in range(1, tiles):
                value = jnp.where(past[t - 1], bandsb[t, k], value)
            coef[k, :, at] = value
        return carry

    lax.fori_loop(0, cols // LANES, coefficients, 0)
    base = 8
    D[0:base, :] = jnp.zeros((base, cols), F32)
    D[base + levels:, :] = jnp.zeros((D.shape[0] - base - levels, cols), F32)

    own_geo.wait()
    for cp in geo_ex:
        cp.wait_recv()
    for g in range(ng):
        for r in range(rows):
            D[base + g * lev:base + (g + 1) * lev, r * hy:(r + 1) * hy] = G[g, r].astype(F32)

    def vertical(q, carry):
        at = pl.ds(pl.multiple_of(q * hy, LANES), hy)
        value = D[base:base + levels, at]
        for k in range(nband):
            value = value + coef[k, :, at] * D[base + k - pad:base + k - pad + levels, at]
        for m in range(nm):
            FS[m, :, at] = value[m * lm:(m + 1) * lm].astype(BF16)
        return carry

    lax.fori_loop(0, cols // hy, vertical, 0)
    filt_ex = [exchange(lambda p: FS.at[p], FR.at[d], fs_sem, fr_sem, "mem", mem, d, nm) for d in range(1, nm)]
    for cp in filt_ex:
        cp.start()
    own_filt = pltpu.make_async_copy(FS.at[mem], FR.at[0], fr_sem.at[0])
    own_filt.start()
    own_pert = pltpu.make_async_copy(PS.at[mem], PR.at[0], pr_sem.at[0])
    own_pert.start()
    own_pert.wait()
    own_filt.wait()
    for cp in pert_ex:
        cp.wait_recv()
    for cp in filt_ex:
        cp.wait_recv()

    def total(q, carry):
        at = pl.ds(pl.multiple_of(q * hy, LANES), hy)
        acc = jnp.zeros((nvar * lm, hy), F32)
        for m in range(nm):
            f = FR[m, :, at].astype(F32)
            acc = acc + PR[m, :, at].astype(F32) * jnp.concatenate([f] * nvar, axis=0)
        for v in range(nvar):
            out[v, :, at] = acc[v * lm:(v + 1) * lm]
        return carry

    lax.fori_loop(0, cols // hy, total, 0)
    for cp in pert_ex + geo_ex + filt_ex:
        cp.wait_send()


def body(nm, ng, control, kappa_table, kappa_index, tile_bounds, filter_bands, perturbation):
    _, lev, hx, hy = control.shape
    nvar, _, levels, cols = perturbation.shape
    lm = levels // nm
    rows = hx // ng
    tiles, nband, _ = filter_bands.shape
    dma = pltpu.SemaphoreType.DMA
    hbm = pl.BlockSpec(memory_space=pl.ANY)
    return pl.pallas_call(
        functools.partial(kernel, nm, ng),
        out_shape=jax.ShapeDtypeStruct((nvar, lm, cols), F32),
        in_specs=[hbm] * 6,
        out_specs=pl.BlockSpec(memory_space=pltpu.VMEM),
        scratch_shapes=[
            pltpu.SMEM(kappa_table.shape, F32),
            pltpu.SMEM(tile_bounds.shape, jnp.int32),
            pltpu.VMEM((hx, lev, hy), F32),
            pltpu.VMEM((hx, lev, hy), F32),
            pltpu.VMEM((hx, lev, hy), F32),
            pltpu.VMEM((hx, lev, LANES), F32),
            pltpu.VMEM((hy, hy), BF16),
            pltpu.VMEM((hy, hy), BF16),
            pltpu.VMEM((hx, hy), jnp.int32),
            pltpu.VMEM((hx + 8, hy), F32),
            pltpu.VMEM((nband, tiles, levels), F32),
            pltpu.VMEM((tiles, nband, levels, LANES), F32),
            pltpu.VMEM((nband, levels, cols), F32),
            pltpu.VMEM((nvar, levels, cols), BF16),
            pltpu.VMEM((nm, nvar * lm, cols), BF16),
            pltpu.VMEM((nm, nvar * lm, cols), BF16),
            pltpu.VMEM((hx, lev, hy), BF16),
            pltpu.VMEM((ng, rows, lev, hy), BF16),
            pltpu.VMEM((levels + 16, cols), F32),
            pltpu.VMEM((nm, lm, cols), BF16),
            pltpu.VMEM((nm, lm, cols), BF16),
            dma((5 + lev,)), dma((nm,)), dma((nm,)), dma((ng,)), dma((ng,)), dma((nm,)), dma((nm,)),
        ],
        compiler_params=pltpu.CompilerParams(
            collective_id=0, has_side_effects=True, vmem_limit_bytes=56 * 2**20),
    )(control, kappa_table, kappa_index, tile_bounds, jnp.swapaxes(filter_bands, 0, 1), perturbation)


def solution(mesh):
    in_specs = (P("mem", "geo", None, None), P(), P(), P(), P(), P(None, "mem", None, "geo"))
    out_specs = P(None, "mem", "geo")
    run = functools.partial(body, mesh.shape["mem"], mesh.shape["geo"])
    return jax.shard_map(run, mesh=mesh, in_specs=in_specs, out_specs=out_specs, check_vma=False)
```

```python
import functools

import jax
import jax.numpy as jnp
from jax import lax
from jax.experimental import pallas as pl
from jax.experimental.pallas import tpu as pltpu
from jax.sharding import PartitionSpec as P

ITERS = 10
F32, BF16 = jnp.float32, jnp.bfloat16
LANES = 128


def kernel(nm, ng, ctrl, table_hbm, kidx_hbm, bounds_hbm, bands_hbm, pert_hbm, out,
           table, bounds, S, WE, WN, WS, spread, gather, kidx, kf, bands, bandsb, coef, pert, PS, PR, B, G, D, FS, FR, XS, XR,
           loc_sem, ps_sem, pr_sem, gs_sem, gr_sem, fs_sem, fr_sem, xs_sem, xr_sem):
    mem = lax.axis_index("mem")
    geo = lax.axis_index("geo")
    hx, lev, hy = S.shape
    nvar, levels, cols = pert.shape
    lm = levels // nm
    rows = hx // ng
    nband, tiles, _ = bands.shape
    parts = hy // LANES
    head = FS.shape[2]
    pad = nband // 2

    barrier = pltpu.get_barrier_semaphore()
    for d in range(1, nm):
        pl.semaphore_signal(barrier, inc=1, device_id={"mem": lax.rem(mem + d, nm)}, device_id_type=pl.DeviceIdType.MESH)
    for d in range(1, ng):
        pl.semaphore_signal(barrier, inc=1, device_id={"geo": lax.rem(geo + d, ng)}, device_id_type=pl.DeviceIdType.MESH)

    pert_cp = pltpu.make_async_copy(pert_hbm.at[:, 0], pert, loc_sem.at[0])
    pert_cp.start()
    kidx_cp = pltpu.make_async_copy(kidx_hbm, kidx, loc_sem.at[1])
    kidx_cp.start()
    bands_cp = pltpu.make_async_copy(bands_hbm, bands, loc_sem.at[2])
    bands_cp.start()
    table_cp = pltpu.make_async_copy(table_hbm, table, loc_sem.at[3])
    table_cp.start()
    bounds_cp = pltpu.make_async_copy(bounds_hbm, bounds, loc_sem.at[4])
    bounds_cp.start()
    ctrl_cps = []
    for l in range(lev):
        cp = pltpu.make_async_copy(ctrl.at[0, l], S.at[:, l], loc_sem.at[5 + l])
        cp.start()
        ctrl_cps.append(cp)

    left = lax.broadcasted_iota(jnp.int32, (hy, hy), 0)
    right = lax.broadcasted_iota(jnp.int32, (hy, hy), 1)
    spread[...] = jnp.where(left == (right % LANES) * parts + right // LANES, 1.0, 0.0).astype(BF16)
    gather[...] = jnp.where(right == (left % LANES) * parts + left // LANES, 1.0, 0.0).astype(BF16)

    pert_cp.wait()

    def repack(q, carry):
        at = pl.ds(pl.multiple_of(q * hy, LANES), hy)
        vals = [pert[v, :, at].astype(F32) for v in range(nvar)]
        for m in range(nm):
            piece = jnp.concatenate([v[m * lm:(m + 1) * lm] for v in vals], axis=0)
            PS[m, :, at] = piece.astype(BF16)
        return carry

    lax.fori_loop(0, head // hy, repack, 0)
    pl.semaphore_wait(barrier, nm - 1 + ng - 1)

    def exchange(src, dst, send, recv, axis, me, d, n):
        peer = lax.rem(me + d, n)
        return pltpu.make_async_remote_copy(
            src_ref=src(peer), dst_ref=dst, send_sem=send.at[d], recv_sem=recv.at[d],
            device_id={axis: peer}, device_id_type=pl.DeviceIdType.MESH)

    pert_ex = [exchange(lambda p: PS.at[p], PR.at[d], ps_sem, pr_sem, "mem", mem, d, nm) for d in range(1, nm)]
    for cp in pert_ex:
        cp.start()

    kidx_cp.wait()
    table_cp.wait()
    index = jnp.dot(kidx[...].astype(F32).astype(BF16), spread[...], preferred_element_type=F32)
    field = jnp.zeros(index.shape, F32)
    for entry in range(table.shape[0]):
        field = jnp.where(index == float(entry), table[entry], field)
    kf[0:hx] = field
    kf[hx:] = jnp.zeros((kf.shape[0] - hx, hy), F32)
    east = 0.5 * (field + kf[1:hx + 1])
    lane = lax.broadcasted_iota(jnp.int32, (hx, LANES), 1)
    cut = [field[:, p * LANES:(p + 1) * LANES] for p in range(parts)]
    norths = [0.5 * (cut[p] + cut[p + 1]) for p in range(parts - 1)]
    last = 0.5 * (cut[-1] + pltpu.roll(cut[0], LANES - 1, axis=1))
    norths.append(jnp.where(lane < LANES - 1, last, 0.0))
    south = pltpu.roll(norths[-1], 1, axis=1)
    for i in range(hx):
        if i < hx - 1:
            WE[i] = jnp.broadcast_to(east[i:i + 1], (lev, hy))
        for p in range(parts):
            WN[i, :, p * LANES:(p + 1) * LANES] = jnp.broadcast_to(norths[p][i:i + 1], (lev, LANES))
        WS[i] = jnp.broadcast_to(south[i:i + 1], (lev, LANES))

    for cp in ctrl_cps:
        cp.wait()
    group = rows if (rows * lev) % 8 == 0 else hx
    for i in range(0, hx, group):
        x = S[i:i + group].reshape(group * lev, hy)
        high = x.astype(BF16)
        low = (x - high.astype(F32)).astype(BF16)
        x = (jnp.dot(high, spread[...], preferred_element_type=F32)
             + jnp.dot(low, spread[...], preferred_element_type=F32))
        S[i:i + group] = x.reshape(group, lev, hy)

    def step(it, carry):
        s = [S[0, :, p * LANES:(p + 1) * LANES] for p in range(parts)]
        before = None
        for i in range(hx):
            wn = [WN[i, :, p * LANES:(p + 1) * LANES] for p in range(parts)]
            ahead = s[1:] + [pltpu.roll(s[0], LANES - 1, axis=1)]
            flux = [wn[p] * (ahead[p] - s[p]) for p in range(parts)]
            behind = [WS[i] * (s[0] - pltpu.roll(s[-1], 1, axis=1))] + flux[:-1]
            new = [s[p] + (flux[p] - behind[p]) for p in range(parts)]
            if before is not None:
                new = [new[p] - before[p] for p in range(parts)]
            if i < hx - 1:
                after = [S[i + 1, :, p * LANES:(p + 1) * LANES] for p in range(parts)]
                before = [WE[i, :, p * LANES:(p + 1) * LANES] * (after[p] - s[p]) for p in range(parts)]
                new = [new[p] + before[p] for p in range(parts)]
                s = after
            for p in range(parts):
                S[i, :, p * LANES:(p + 1) * LANES] = new[p]
        return carry

    lax.fori_loop(0, ITERS, step, 0)
    for i in range(0, hx, group):
        x = S[i:i + group].reshape(group * lev, hy).astype(BF16)
        x = jnp.dot(x, gather[...], preferred_element_type=F32)
        B[i:i + group] = x.reshape(group, lev, hy).astype(BF16)

    geo_ex = [exchange(lambda p: B.at[pl.ds(p * rows, rows)], G.at[geo], gs_sem, gr_sem, "geo", geo, d, ng)
              for d in range(1, ng)]
    for cp in geo_ex:
        cp.start()
    own_geo = pltpu.make_async_copy(B.at[pl.ds(geo * rows, rows)], G.at[geo], gr_sem.at[0])
    own_geo.start()

    bands_cp.wait()
    bounds_cp.wait()
    eye = (lax.broadcasted_iota(jnp.int32, (levels, levels), 0)
           == lax.broadcasted_iota(jnp.int32, (levels, levels), 1))
    for t in range(tiles):
        for k in range(nband):
            row = jnp.broadcast_to(bands[k, t:t + 1, :], (levels, levels))
            column = jnp.sum(jnp.where(eye, row, 0.0), axis=1, keepdims=True)
            bandsb[t, k] = jnp.broadcast_to(column, (levels, LANES))

    def coefficients(q, carry):
        at = pl.ds(pl.multiple_of(q * LANES, LANES), LANES)
        column = geo * cols + q * LANES + lax.broadcasted_iota(jnp.int32, (levels, LANES), 1)
        past = [column >= bounds[t] for t in range(1, tiles)]
        for k in range(nband):
            value = bandsb[0, k]
            for t in range(1, tiles):
                value = jnp.where(past[t - 1], bandsb[t, k], value)
            coef[k, :, at] = value
        return carry

    lax.fori_loop(0, cols // LANES, coefficients, 0)
    base = 8
    D[0:base, :] = jnp.zeros((base, cols), F32)
    D[base + levels:, :] = jnp.zeros((D.shape[0] - base - levels, cols), F32)

    own_geo.wait()
    for cp in geo_ex:
        cp.wait_recv()
    for g in range(ng):
        for r in range(rows):
            D[base + g * lev:base + (g + 1) * lev, r * hy:(r + 1) * hy] = G[g, r].astype(F32)

    def filtered(q):
        at = pl.ds(pl.multiple_of(q * hy, LANES), hy)
        value = D[base:base + levels, at]
        for k in range(nband):
            value = value + coef[k, :, at] * D[base + k - pad:base + k - pad + levels, at]
        return value.astype(BF16), at

    def vertical(q, carry):
        value, at = filtered(q)
        value = value.astype(F32)
        for m in range(nm):
            FS[m, :, at] = value[m * lm:(m + 1) * lm].astype(BF16)
        return carry

    lax.fori_loop(0, head // hy, vertical, 0)
    filt_ex = [exchange(lambda p: FS.at[p], FR.at[d], fs_sem, fr_sem, "mem", mem, d, nm) for d in range(1, nm)]
    for cp in filt_ex:
        cp.start()

    def products(q, carry):
        value, at = filtered(q)
        to = pl.ds(pl.multiple_of(q * hy - head, LANES), hy)
        vals = [pert[v, :, at].astype(F32) * value.astype(F32) for v in range(nvar)]
        for m in range(nm):
            piece = jnp.concatenate([v[m * lm:(m + 1) * lm] for v in vals], axis=0)
            XS[m, :, to] = piece.astype(BF16)
        return carry

    lax.fori_loop(head // hy, cols // hy, products, 0)
    prod_ex = [exchange(lambda p: XS.at[p], XR.at[d], xs_sem, xr_sem, "mem", mem, d, nm) for d in range(1, nm)]
    for cp in prod_ex:
        cp.start()
    own = [pltpu.make_async_copy(PS.at[mem], PR.at[0], pr_sem.at[0]),
           pltpu.make_async_copy(FS.at[mem], FR.at[0], fr_sem.at[0]),
           pltpu.make_async_copy(XS.at[mem], XR.at[0], xr_sem.at[0])]
    for cp in own:
        cp.start()
    for cp in own:
        cp.wait()
    for cp in pert_ex:
        cp.wait_recv()
    for cp in filt_ex:
        cp.wait_recv()

    def total(q, carry):
        at = pl.ds(pl.multiple_of(q * hy, LANES), hy)
        acc = jnp.zeros((nvar * lm, hy), F32)
        for m in range(nm):
            f = FR[m, :, at].astype(F32)
            acc = acc + PR[m, :, at].astype(F32) * jnp.concatenate([f] * nvar, axis=0)
        for v in range(nvar):
            out[v, :, at] = acc[v * lm:(v + 1) * lm]
        return carry

    lax.fori_loop(0, head // hy, total, 0)
    for cp in prod_ex:
        cp.wait_recv()

    def total_products(q, carry):
        at = pl.ds(pl.multiple_of(q * hy, LANES), hy)
        acc = XR[0, :, pl.ds(pl.multiple_of(q * hy - head, LANES), hy)].astype(F32)
        for m in range(1, nm):
            acc = acc + XR[m, :, pl.ds(pl.multiple_of(q * hy - head, LANES), hy)].astype(F32)
        for v in range(nvar):
            out[v, :, at] = acc[v * lm:(v + 1) * lm]
        return carry

    lax.fori_loop(head // hy, cols // hy, total_products, 0)
    for cp in pert_ex + geo_ex + filt_ex + prod_ex:
        cp.wait_send()


def body(nm, ng, control, kappa_table, kappa_index, tile_bounds, filter_bands, perturbation):
    _, lev, hx, hy = control.shape
    nvar, _, levels, cols = perturbation.shape
    lm = levels // nm
    rows = hx // ng
    tiles, nband, _ = filter_bands.shape
    head = cols - max(1, rows // 4) * hy
    dma = pltpu.SemaphoreType.DMA
    hbm = pl.BlockSpec(memory_space=pl.ANY)
    return pl.pallas_call(
        functools.partial(kernel, nm, ng),
        out_shape=jax.ShapeDtypeStruct((nvar, lm, cols), F32),
        in_specs=[hbm] * 6,
        out_specs=pl.BlockSpec(memory_space=pltpu.VMEM),
        scratch_shapes=[
            pltpu.SMEM(kappa_table.shape, F32),
            pltpu.SMEM(tile_bounds.shape, jnp.int32),
            pltpu.VMEM((hx, lev, hy), F32),
            pltpu.VMEM((hx, lev, hy), F32),
            pltpu.VMEM((hx, lev, hy), F32),
            pltpu.VMEM((hx, lev, LANES), F32),
            pltpu.VMEM((hy, hy), BF16),
            pltpu.VMEM((hy, hy), BF16),
            pltpu.VMEM((hx, hy), jnp.int32),
            pltpu.VMEM((hx + 8, hy), F32),
            pltpu.VMEM((nband, tiles, levels), F32),
            pltpu.VMEM((tiles, nband, levels, LANES), F32),
            pltpu.VMEM((nband, levels, cols), F32),
            pltpu.VMEM((nvar, levels, cols), BF16),
            pltpu.VMEM((nm, nvar * lm, head), BF16),
            pltpu.VMEM((nm, nvar * lm, head), BF16),
            pltpu.VMEM((hx, lev, hy), BF16),
            pltpu.VMEM((ng, rows, lev, hy), BF16),
            pltpu.VMEM((levels + 16, cols), F32),
            pltpu.VMEM((nm, lm, head), BF16),
            pltpu.VMEM((nm, lm, head), BF16),
            pltpu.VMEM((nm, nvar * lm, cols - head), BF16),
            pltpu.VMEM((nm, nvar * lm, cols - head), BF16),
            dma((5 + lev,)), dma((nm,)), dma((nm,)), dma((ng,)), dma((ng,)), dma((nm,)), dma((nm,)),
            dma((nm,)), dma((nm,)),
        ],
        compiler_params=pltpu.CompilerParams(
            collective_id=0, has_side_effects=True, vmem_limit_bytes=56 * 2**20),
    )(control, kappa_table, kappa_index, tile_bounds, jnp.swapaxes(filter_bands, 0, 1), perturbation)


def solution(mesh):
    in_specs = (P("mem", "geo", None, None), P(), P(), P(), P(), P(None, "mem", None, "geo"))
    out_specs = P(None, "mem", "geo")
    run = functools.partial(body, mesh.shape["mem"], mesh.shape["geo"])
    return jax.shard_map(run, mesh=mesh, in_specs=in_specs, out_specs=out_specs, check_vma=False)
```

```python
import functools

import jax
import jax.numpy as jnp
from jax import lax
from jax.experimental import pallas as pl
from jax.experimental.pallas import tpu as pltpu
from jax.sharding import PartitionSpec as P

ITERS = 10
F32, BF16 = jnp.float32, jnp.bfloat16
LANES = 128


def kernel(nm, ng, ctrl, table_hbm, kidx_hbm, bounds_hbm, bands_hbm, pert_hbm, out,
           table, bounds, S, WE, WN, WS, spread, gather, kidx, kf, bands, bandsb, coef, pert, PS, PR, B, G, D, FS, FR, XS, XR,
           loc_sem, ps_sem, pr_sem, gs_sem, gr_sem, fs_sem, fr_sem, xs_sem, xr_sem):
    mem = lax.axis_index("mem")
    geo = lax.axis_index("geo")
    hx, lev, hy = S.shape
    nvar, levels, cols = pert.shape
    lm = levels // nm
    rows = hx // ng
    nband, tiles, _ = bands.shape
    parts = hy // LANES
    head = FS.shape[2]
    pad = nband // 2

    far_first = sorted(range(1, nm), key=lambda d: abs(2 * d - nm))
    barrier = pltpu.get_barrier_semaphore()
    for d in range(1, nm):
        pl.semaphore_signal(barrier, inc=1, device_id={"mem": lax.rem(mem + d, nm)}, device_id_type=pl.DeviceIdType.MESH)
    for d in range(1, ng):
        pl.semaphore_signal(barrier, inc=1, device_id={"geo": lax.rem(geo + d, ng)}, device_id_type=pl.DeviceIdType.MESH)

    pert_cp = pltpu.make_async_copy(pert_hbm.at[:, 0], pert, loc_sem.at[0])
    pert_cp.start()
    kidx_cp = pltpu.make_async_copy(kidx_hbm, kidx, loc_sem.at[1])
    kidx_cp.start()
    bands_cp = pltpu.make_async_copy(bands_hbm, bands, loc_sem.at[2])
    bands_cp.start()
    table_cp = pltpu.make_async_copy(table_hbm, table, loc_sem.at[3])
    table_cp.start()
    bounds_cp = pltpu.make_async_copy(bounds_hbm, bounds, loc_sem.at[4])
    bounds_cp.start()
    ctrl_cps = []
    for l in range(lev):
        cp = pltpu.make_async_copy(ctrl.at[0, l], S.at[:, l], loc_sem.at[5 + l])
        cp.start()
        ctrl_cps.append(cp)

    left = lax.broadcasted_iota(jnp.int32, (hy, hy), 0)
    right = lax.broadcasted_iota(jnp.int32, (hy, hy), 1)
    spread[...] = jnp.where(left == (right % LANES) * parts + right // LANES, 1.0, 0.0).astype(BF16)
    gather[...] = jnp.where(right == (left % LANES) * parts + left // LANES, 1.0, 0.0).astype(BF16)

    pert_cp.wait()

    def repack(q, carry):
        at = pl.ds(pl.multiple_of(q * hy, LANES), hy)
        vals = [pert[v, :, at].astype(F32) for v in range(nvar)]
        for m in range(nm):
            piece = jnp.concatenate([v[m * lm:(m + 1) * lm] for v in vals], axis=0)
            PS[m, :, at] = piece.astype(BF16)
        return carry

    lax.fori_loop(0, head // hy, repack, 0)
    pl.semaphore_wait(barrier, nm - 1 + ng - 1)

    def exchange(src, dst, send, recv, axis, me, d, n):
        peer = lax.rem(me + d, n)
        return pltpu.make_async_remote_copy(
            src_ref=src(peer), dst_ref=dst, send_sem=send.at[d], recv_sem=recv.at[d],
            device_id={axis: peer}, device_id_type=pl.DeviceIdType.MESH)

    pert_ex = [exchange(lambda p: PS.at[p], PR.at[d], ps_sem, pr_sem, "mem", mem, d, nm) for d in far_first]
    for cp in pert_ex:
        cp.start()

    kidx_cp.wait()
    table_cp.wait()
    index = jnp.dot(kidx[...].astype(F32).astype(BF16), spread[...], preferred_element_type=F32)
    field = jnp.zeros(index.shape, F32)
    for entry in range(table.shape[0]):
        field = jnp.where(index == float(entry), table[entry], field)
    kf[0:hx] = field
    kf[hx:] = jnp.zeros((kf.shape[0] - hx, hy), F32)
    east = 0.5 * (field + kf[1:hx + 1])
    lane = lax.broadcasted_iota(jnp.int32, (hx, LANES), 1)
    cut = [field[:, p * LANES:(p + 1) * LANES] for p in range(parts)]
    norths = [0.5 * (cut[p] + cut[p + 1]) for p in range(parts - 1)]
    last = 0.5 * (cut[-1] + pltpu.roll(cut[0], LANES - 1, axis=1))
    norths.append(jnp.where(lane < LANES - 1, last, 0.0))
    south = pltpu.roll(norths[-1], 1, axis=1)
    for i in range(hx):
        if i < hx - 1:
            WE[i] = jnp.broadcast_to(east[i:i + 1], (lev, hy))
        for p in range(parts):
            WN[i, :, p * LANES:(p + 1) * LANES] = jnp.broadcast_to(norths[p][i:i + 1], (lev, LANES))
        WS[i] = jnp.broadcast_to(south[i:i + 1], (lev, LANES))

    for cp in ctrl_cps:
        cp.wait()
    group = rows if (rows * lev) % 8 == 0 else hx
    for i in range(0, hx, group):
        x = S[i:i + group].reshape(group * lev, hy)
        high = x.astype(BF16)
        low = (x - high.astype(F32)).astype(BF16)
        x = (jnp.dot(high, spread[...], preferred_element_type=F32)
             + jnp.dot(low, spread[...], preferred_element_type=F32))
        S[i:i + group] = x.reshape(group, lev, hy)

    def step(it, carry):
        s = [S[0, :, p * LANES:(p + 1) * LANES] for p in range(parts)]
        before = None
        for i in range(hx):
            wn = [WN[i, :, p * LANES:(p + 1) * LANES] for p in range(parts)]
            ahead = s[1:] + [pltpu.roll(s[0], LANES - 1, axis=1)]
            flux = [wn[p] * (ahead[p] - s[p]) for p in range(parts)]
            behind = [WS[i] * (s[0] - pltpu.roll(s[-1], 1, axis=1))] + flux[:-1]
            new = [s[p] + (flux[p] - behind[p]) for p in range(parts)]
            if before is not None:
                new = [new[p] - before[p] for p in range(parts)]
            if i < hx - 1:
                after = [S[i + 1, :, p * LANES:(p + 1) * LANES] for p in range(parts)]
                before = [WE[i, :, p * LANES:(p + 1) * LANES] * (after[p] - s[p]) for p in range(parts)]
                new = [new[p] + before[p] for p in range(parts)]
                s = after
            for p in range(parts):
                S[i, :, p * LANES:(p + 1) * LANES] = new[p]
        return carry

    lax.fori_loop(0, ITERS, step, 0)
    for i in range(0, hx, group):
        x = S[i:i + group].reshape(group * lev, hy).astype(BF16)
        x = jnp.dot(x, gather[...], preferred_element_type=F32)
        B[i:i + group] = x.reshape(group, lev, hy).astype(BF16)

    geo_ex = [exchange(lambda p: B.at[pl.ds(p * rows, rows)], G.at[geo], gs_sem, gr_sem, "geo", geo, d, ng)
              for d in range(1, ng)]
    for cp in geo_ex:
        cp.start()
    own_geo = pltpu.make_async_copy(B.at[pl.ds(geo * rows, rows)], G.at[geo], gr_sem.at[0])
    own_geo.start()

    bands_cp.wait()
    bounds_cp.wait()
    eye = (lax.broadcasted_iota(jnp.int32, (levels, levels), 0)
           == lax.broadcasted_iota(jnp.int32, (levels, levels), 1))
    for t in range(tiles):
        for k in range(nband):
            row = jnp.broadcast_to(bands[k, t:t + 1, :], (levels, levels))
            column = jnp.sum(jnp.where(eye, row, 0.0), axis=1, keepdims=True)
            bandsb[t, k] = jnp.broadcast_to(column, (levels, LANES))

    def coefficients(q, carry):
        at = pl.ds(pl.multiple_of(q * LANES, LANES), LANES)
        column = geo * cols + q * LANES + lax.broadcasted_iota(jnp.int32, (levels, LANES), 1)
        past = [column >= bounds[t] for t in range(1, tiles)]
        for k in range(nband):
            value = bandsb[0, k]
            for t in range(1, tiles):
                value = jnp.where(past[t - 1], bandsb[t, k], value)
            coef[k, :, at] = value
        return carry

    lax.fori_loop(0, cols // LANES, coefficients, 0)
    base = 8
    D[0:base, :] = jnp.zeros((base, cols), F32)
    D[base + levels:, :] = jnp.zeros((D.shape[0] - base - levels, cols), F32)

    own_geo.wait()
    for cp in geo_ex:
        cp.wait_recv()
    for g in range(ng):
        for r in range(rows):
            D[base + g * lev:base + (g + 1) * lev, r * hy:(r + 1) * hy] = G[g, r].astype(F32)

    def filtered(q):
        at = pl.ds(pl.multiple_of(q * hy, LANES), hy)
        value = D[base:base + levels, at]
        for k in range(nband):
            value = value + coef[k, :, at] * D[base + k - pad:base + k - pad + levels, at]
        return value.astype(BF16), at

    def vertical(q, carry):
        value, at = filtered(q)
        value = value.astype(F32)
        for m in range(nm):
            FS[m, :, at] = value[m * lm:(m + 1) * lm].astype(BF16)
        return carry

    lax.fori_loop(0, head // hy, vertical, 0)
    filt_ex = [exchange(lambda p: FS.at[p], FR.at[d], fs_sem, fr_sem, "mem", mem, d, nm) for d in far_first]
    for cp in filt_ex:
        cp.start()

    def products(q, carry):
        value, at = filtered(q)
        to = pl.ds(pl.multiple_of(q * hy - head, LANES), hy)
        vals = [pert[v, :, at].astype(F32) * value.astype(F32) for v in range(nvar)]
        for m in range(nm):
            piece = jnp.concatenate([v[m * lm:(m + 1) * lm] for v in vals], axis=0)
            XS[m, :, to] = piece.astype(BF16)
        return carry

    lax.fori_loop(head // hy, cols // hy, products, 0)
    prod_ex = [exchange(lambda p: XS.at[p], XR.at[d], xs_sem, xr_sem, "mem", mem, d, nm) for d in far_first]
    for cp in prod_ex:
        cp.start()
    own = [pltpu.make_async_copy(PS.at[mem], PR.at[0], pr_sem.at[0]),
           pltpu.make_async_copy(FS.at[mem], FR.at[0], fr_sem.at[0]),
           pltpu.make_async_copy(XS.at[mem], XR.at[0], xr_sem.at[0])]
    for cp in own:
        cp.start()
    for cp in own:
        cp.wait()
    for cp in pert_ex:
        cp.wait_recv()
    for cp in filt_ex:
        cp.wait_recv()

    def total(q, carry):
        at = pl.ds(pl.multiple_of(q * hy, LANES), hy)
        acc = jnp.zeros((nvar * lm, hy), F32)
        for m in range(nm):
            f = FR[m, :, at].astype(F32)
            acc = acc + PR[m, :, at].astype(F32) * jnp.concatenate([f] * nvar, axis=0)
        for v in range(nvar):
            out[v, :, at] = acc[v * lm:(v + 1) * lm]
        return carry

    lax.fori_loop(0, head // hy, total, 0)
    for cp in prod_ex:
        cp.wait_recv()

    def total_products(q, carry):
        at = pl.ds(pl.multiple_of(q * hy, LANES), hy)
        acc = XR[0, :, pl.ds(pl.multiple_of(q * hy - head, LANES), hy)].astype(F32)
        for m in range(1, nm):
            acc = acc + XR[m, :, pl.ds(pl.multiple_of(q * hy - head, LANES), hy)].astype(F32)
        for v in range(nvar):
            out[v, :, at] = acc[v * lm:(v + 1) * lm]
        return carry

    lax.fori_loop(head // hy, cols // hy, total_products, 0)
    for cp in pert_ex + geo_ex + filt_ex + prod_ex:
        cp.wait_send()


def body(nm, ng, control, kappa_table, kappa_index, tile_bounds, filter_bands, perturbation):
    _, lev, hx, hy = control.shape
    nvar, _, levels, cols = perturbation.shape
    lm = levels // nm
    rows = hx // ng
    tiles, nband, _ = filter_bands.shape
    head = cols - max(1, rows // 4) * hy
    dma = pltpu.SemaphoreType.DMA
    hbm = pl.BlockSpec(memory_space=pl.ANY)
    return pl.pallas_call(
        functools.partial(kernel, nm, ng),
        out_shape=jax.ShapeDtypeStruct((nvar, lm, cols), F32),
        in_specs=[hbm] * 6,
        out_specs=pl.BlockSpec(memory_space=pltpu.VMEM),
        scratch_shapes=[
            pltpu.SMEM(kappa_table.shape, F32),
            pltpu.SMEM(tile_bounds.shape, jnp.int32),
            pltpu.VMEM((hx, lev, hy), F32),
            pltpu.VMEM((hx, lev, hy), F32),
            pltpu.VMEM((hx, lev, hy), F32),
            pltpu.VMEM((hx, lev, LANES), F32),
            pltpu.VMEM((hy, hy), BF16),
            pltpu.VMEM((hy, hy), BF16),
            pltpu.VMEM((hx, hy), jnp.int32),
            pltpu.VMEM((hx + 8, hy), F32),
            pltpu.VMEM((nband, tiles, levels), F32),
            pltpu.VMEM((tiles, nband, levels, LANES), F32),
            pltpu.VMEM((nband, levels, cols), F32),
            pltpu.VMEM((nvar, levels, cols), BF16),
            pltpu.VMEM((nm, nvar * lm, head), BF16),
            pltpu.VMEM((nm, nvar * lm, head), BF16),
            pltpu.VMEM((hx, lev, hy), BF16),
            pltpu.VMEM((ng, rows, lev, hy), BF16),
            pltpu.VMEM((levels + 16, cols), F32),
            pltpu.VMEM((nm, lm, head), BF16),
            pltpu.VMEM((nm, lm, head), BF16),
            pltpu.VMEM((nm, nvar * lm, cols - head), BF16),
            pltpu.VMEM((nm, nvar * lm, cols - head), BF16),
            dma((5 + lev,)), dma((nm,)), dma((nm,)), dma((ng,)), dma((ng,)), dma((nm,)), dma((nm,)),
            dma((nm,)), dma((nm,)),
        ],
        compiler_params=pltpu.CompilerParams(
            collective_id=0, has_side_effects=True, vmem_limit_bytes=56 * 2**20),
    )(control, kappa_table, kappa_index, tile_bounds, jnp.swapaxes(filter_bands, 0, 1), perturbation)


def solution(mesh):
    in_specs = (P("mem", "geo", None, None), P(), P(), P(), P(), P(None, "mem", None, "geo"))
    out_specs = P(None, "mem", "geo")
    run = functools.partial(body, mesh.shape["mem"], mesh.shape["geo"])
    return jax.shard_map(run, mesh=mesh, in_specs=in_specs, out_specs=out_specs, check_vma=False)
```
